32 devices in a mesh: inst: 4 (over y, x), scen: 8 (over z, core).
Axes of the slice: x: 2, y: 2, z: 4, core: 2. Of those that a mesh axis runs over, the one named last changes fastest.
Arguments:
- positions: int32 [512, 16384], P(None, 'inst'), may hold values from -50 to 50
- holding_block_grid: int32 [8, 128], P(None, 'inst'), may hold values 0 or 1
- risk: float32 [16384, 8192], P('inst', 'scen'), may hold values from -64 to 64
Outputs:
- margin: float32 [512], P('inst')
- gradient: float32 [512, 16384], P('scen', 'inst')
The draws below stay inside these ranges and needn't reach their ends.
All inputs are finite; a program needn't handle non-finite values. No bound on the sum of `holding_block_grid` on one device may be relied on, other than what follows from the above.
Results may differ from the reference program's by a relative error of at most 0.0003.
Values sent between devices are 32-bit elements; how exact they have to be, the bound alone decides.
A program may use at most 64 MiB of HBM per device.

```python
import math
import jax
import jax.numpy as jnp
from jax import lax

ACC = 512
INSTRUMENT_TOTAL = 16384
ABLK = 64
IBLK = 128
SCEN = 8192


def draw_risk(key, part):
    first, second, third = jax.random.split(jax.random.fold_in(key, 17), 3)
    row_scale = jnp.exp(jax.random.uniform(second, (INSTRUMENT_TOTAL, 1), jnp.float32, jnp.log(0.3), jnp.log(3.0)))
    jitter = jnp.exp(jax.random.uniform(third, (1, SCEN), jnp.float32, jnp.log(0.9), jnp.log(1.1)))
    position = jnp.arange(SCEN, dtype=jnp.float32) / SCEN
    base = jnp.clip(jax.random.normal(first, (INSTRUMENT_TOTAL, SCEN), jnp.float32), -6.0, 6.0)
    ramp = jnp.sqrt(1.0 + 2.2 * position)
    result = 0.25 * base * row_scale * (jitter * ramp[None, :])
    return result


def with_ends(values, rng, low, high):
    dims = values.shape
    index_at = [jax.random.randint(jax.random.fold_in(rng, axis), (), 0, dims[axis]) for axis in range(len(dims))]
    values = values.at[tuple(index_at)].set(low)
    longest = dims.index(max(dims))
    index_at[longest] = (index_at[longest] + 1) % dims[longest]
    return values.at[tuple(index_at)].set(high)


def setup_inputs(seed: int = 0) -> dict:
    splits = jax.random.split(jax.random.key(seed), 4)
    return {
        "positions": with_ends(jax.random.randint(splits[0], (ACC, INSTRUMENT_TOTAL), -50, 51), jax.random.fold_in(splits[0], 1), -50, 50).astype(jnp.int32),
        "holding_block_grid": with_ends((jax.random.randint(splits[1], (ACC // ABLK, INSTRUMENT_TOTAL // IBLK), 0, 4) < 3).astype(jnp.int32), jax.random.fold_in(splits[1], 1), 0, 1),
        "risk": draw_risk(jax.random.fold_in(splits[3], 71), 0),
    }


def reference(positions, holding_block_grid, risk):
    live_mask = jnp.repeat(jnp.repeat(holding_block_grid, ABLK, axis=0), IBLK, axis=1)
    held = (positions * live_mask).astype(jnp.float32)
    profit_and_losses = jnp.dot(held, risk, precision=lax.Precision.HIGHEST, preferred_element_type=jnp.float32)
    softness_level = 8.0 * math.sqrt(INSTRUMENT_TOTAL)
    tail_logits = -profit_and_losses / softness_level
    peak = lax.optimization_barrier(jnp.max(tail_logits, axis=1))
    shifted = jnp.exp(tail_logits - peak[:, None])
    total = lax.optimization_barrier(jnp.sum(shifted, axis=1))
    margin = peak + jnp.log(total) - math.log(SCEN)
    weights = shifted / total[:, None]
    gradient = -jnp.einsum('as,is->ai', weights, risk, precision=lax.Precision.HIGHEST)
    return (margin, gradient)
```

```python
import math

import jax
import jax.numpy as jnp
from jax import lax
from jax.sharding import PartitionSpec as P


ABLK = 64
IBLK = 128
CORES = 2


def pick(blocks, which):
    result = blocks[0]
    for k in range(1, len(blocks)):
        result = jnp.where(which == k, blocks[k], result)
    return result


def all_reduce_rows(part, axis):
    size = lax.axis_size(axis)
    me = lax.axis_index(axis)
    rows = part.shape[0] // size
    mine = lax.dynamic_slice_in_dim(part, me * rows, rows)
    for k in range(1, size):
        away = lax.dynamic_slice_in_dim(part, (me ^ k) * rows, rows)
        mine = mine + lax.ppermute(away, axis, [(j, j ^ k) for j in range(size)])
    parts = [mine] + [
        lax.ppermute(mine, axis, [(j, j ^ k) for j in range(size)]) for k in range(1, size)
    ]
    return jnp.concatenate([pick(parts, me ^ j) for j in range(size)])


def body(positions, holding_block_grid, risk):
    accounts, instruments = positions.shape
    inst_number = lax.axis_size("inst")
    scen_number = lax.axis_size("scen")
    chips = scen_number // CORES
    rows = accounts // scen_number
    me = lax.axis_index("scen")
    z, core = me // CORES, me % CORES
    softness_level = 8.0 * math.sqrt(instruments * inst_number)
    total_scen = risk.shape[1] * scen_number

    block_rows, block_cols = holding_block_grid.shape
    live_mask = jnp.broadcast_to(
        holding_block_grid[:, None, :, None], (block_rows, ABLK, block_cols, IBLK)
    ).reshape(accounts, block_cols * IBLK)
    held = (positions * live_mask).astype(jnp.float32)

    span = CORES * rows
    owned = [None] * chips
    peaks = [None] * chips
    totals = [None] * chips
    core_pairs = [(k, k ^ 1) for k in range(scen_number)]
    stride = max(1, chips // 4)
    for start in range(0, chips // 2, stride):
        lows = list(range(start, start + stride))
        where_to = lows + [chips - 1 - q for q in lows]
        held_part = jnp.concatenate([held[q * span : (q + 1) * span] for q in where_to])
        pnl = jnp.dot(
            held_part, risk, precision=lax.Precision.HIGH, preferred_element_type=jnp.float32
        )
        scores = -all_reduce_rows(pnl, "inst") / softness_level
        local_peak = jnp.max(scores, axis=1)
        tails = jnp.exp(scores - local_peak[:, None])
        local_total = jnp.sum(tails, axis=1)
        stats = jnp.stack([local_peak, local_total])
        gathered = [stats] + [
            lax.ppermute(stats, "scen", [(j, j ^ k) for j in range(scen_number)])
            for k in range(1, scen_number)
        ]
        peak = gathered[0][0]
        for other in gathered[1:]:
            peak = jnp.maximum(peak, other[0])
        terms = [other[1] * jnp.exp(other[0] - peak) for other in gathered]
        while len(terms) > 1:
            terms = [a + b for a, b in zip(terms[::2], terms[1::2])]
        total = terms[0]
        factor = -jnp.exp(local_peak - peak) / total
        partial = jnp.einsum("as,is->ai", tails, risk, precision=lax.Precision.HIGH)
        partial = (partial * factor[:, None]).reshape(2 * stride, CORES, rows, instruments)
        peer = jnp.where(core == 0, partial[:, 1], partial[:, 0])
        kept = jnp.where(core == 0, partial[:, 0], partial[:, 1])
        both = kept + lax.ppermute(peer, "scen", core_pairs)
        for side, where in enumerate(where_to):
            owned[where] = both[side]
            peaks[where] = peak[side * span : (side + 1) * span]
            totals[where] = total[side * span : (side + 1) * span]

    def hop(value, senders, step):
        pairs = [(q * CORES + c, (q + step) * CORES + c) for q in senders for c in range(CORES)]
        return lax.ppermute(value, "scen", pairs)

    up = down = None
    for t in range(1, chips):
        send_up = pick(owned[chips - t :], z)
        send_down = pick(owned[:t][::-1], chips - 1 - z)
        if t > 1:
            send_up = send_up + up
            send_down = send_down + down
        up = hop(send_up, range(t), 1)
        down = hop(send_down, range(chips - t, chips), -1)
    gradient = pick(owned, z) + up + down

    peak = jnp.concatenate(peaks)
    total = jnp.concatenate(totals)
    margin = peak + jnp.log(total) - math.log(total_scen)
    share = accounts // inst_number
    margin = lax.dynamic_slice_in_dim(margin, lax.axis_index("inst") * share, share)
    return (margin, gradient)


def solution(mesh):
    placed = (P(None, "inst"), P(None, "inst"), P("inst", "scen"))
    return jax.shard_map(
        body, mesh=mesh, in_specs=placed, out_specs=(P("inst"), P("scen", "inst")), check_vma=False
    )
```
